256 devices in a mesh: sector: 16 (over y, x), obl: 16 (over z, core).
Axes of the slice: x: 4, y: 4, z: 8, core: 2. Of those that a mesh axis runs over, the one named last changes fastest.
Arguments:
- spectrum: float32 [2, 8, 32, 65536], P(None, None, 'sector', 'obl'), may hold values from -6 to 6
- quantile_index: int32 [8], replicated, may hold values from 32768 to 64512
- bands: int32 [1048576], P(('sector', 'obl')), may hold values from 1 to 1024
- default_prob: float32 [1048576], P(('sector', 'obl')), may hold values from 0.002 to 0.1
- weights: int32 [32, 1048576], P(None, ('sector', 'obl')), may hold values from 0 to 8
- live_rows: int32 [16, 16], P('sector', 'obl'), may hold values from 1 to 4096, as said below
Outputs:
- obligor_contrib: float32 [8, 1048576], P(None, ('sector', 'obl'))
- sector_share: float32 [8, 32], P(None, 'sector')
The draws below stay inside these ranges and needn't reach their ends.
Inputs may be any that keep to these rules, and one draw needn't show every extreme that they name: `live_rows`: in each row (the devices of one sector index), the entries sum to 16384; exactly one of them equals 4096.
All inputs are finite; a program needn't handle non-finite values.
Results may differ from the reference program's by a relative error of at most 0.00011.
Values sent between devices are 32-bit elements; how exact they have to be, the bound alone decides.
No kernel may reach another device: no remote copies, remote signals or barrier semaphores. Data moves between devices by JAX's collectives and lax.ppermute only.
A program may use at most 64 MiB of HBM per device.

```python
import math
import jax
import jax.numpy as jnp
from jax import lax

GRID = 65536
BANDS = 1024
SCEN = 8
SECTORS = 32
OBL_DEV = 1024
CAP = 4096
SLOTS = 1048576
OBLIGORS = 262144
N_SECTOR = 16
N_OBL = 16


def draw_live_rows(key, part):
    heavy_key, share_key = jax.random.split(jax.random.fold_in(key, 17))
    heavy_index = jax.random.randint(heavy_key, (N_SECTOR, 1), 0, N_OBL)
    spread = jax.random.randint(share_key, (N_SECTOR, N_OBL), 500, 1001)
    column = jnp.arange(N_OBL, dtype=jnp.int32)[None, :]
    is_heavy = column == heavy_index
    spread = jnp.where(is_heavy, 0, spread)
    remainder_rows = (N_OBL - 4) * OBL_DEV
    base_rows = 1 + (remainder_rows - (N_OBL - 1)) * spread // jnp.sum(spread, axis=1, keepdims=True)
    base_rows = jnp.where(is_heavy, 0, base_rows)
    leftover = remainder_rows - jnp.sum(base_rows, axis=1, keepdims=True)
    position = jnp.cumsum(jnp.where(is_heavy, 0, 1), axis=1) - 1
    extra_row = jnp.where(is_heavy, 0, (position < leftover).astype(jnp.int32))
    return jnp.where(is_heavy, 4 * OBL_DEV, base_rows + extra_row).astype(jnp.int32)


def with_ends(values, own_key, least, top_value):
    index_at = [jax.random.randint(jax.random.fold_in(own_key, axis), (), 0, length) for axis, length in enumerate(values.shape)]
    longest = values.shape.index(max(values.shape))
    beside = index_at[:longest] + [(index_at[longest] + 1) % values.shape[longest]] + index_at[longest + 1:]
    return values.at[tuple(index_at)].set(least).at[tuple(beside)].set(top_value)


def block_levels(own_key, dims, cuts, least, largest):
    gain, own = 1.0, jax.random.fold_in(own_key, 6)
    for axis_at, blocks in cuts:
        draws = jnp.exp(jax.random.uniform(jax.random.fold_in(own, axis_at), (blocks,), jnp.float32, least / len(cuts), largest / len(cuts)))
        gain = gain * jnp.repeat(draws, dims[axis_at] // blocks).reshape([-1 if axis == axis_at else 1 for axis in range(len(dims))])
    return gain


def normal_values(stream_key, extent, scale, limit, pieces=(), kind=jnp.bfloat16):
    factor_of = block_levels(stream_key, extent, pieces, -0.22, 0.18) if pieces else 1.0
    values = jax.random.normal(stream_key, extent, jnp.float32) * scale * factor_of
    return jnp.minimum(jnp.maximum(values, -limit), limit).astype(kind)


def setup_inputs(seed: int = 0) -> dict:
    streams_of = jax.random.split(jax.random.key(seed), 7)
    spectrum = normal_values(streams_of[0], (2, SCEN, SECTORS, GRID), 1.0, 6.0, ((2, 16), (3, 16)), jnp.float32)
    quantile_index = with_ends(jax.random.randint(streams_of[1], (SCEN,), GRID // 2, GRID - BANDS + 1), jax.random.fold_in(streams_of[1], 1), GRID // 2, GRID - BANDS).astype(jnp.int32)
    bands = with_ends(jax.random.randint(streams_of[2], (SLOTS,), 1, BANDS + 1), jax.random.fold_in(streams_of[2], 1), 1, BANDS).astype(jnp.int32)
    default_prob = jnp.clip(jnp.exp(math.log(0.1) - 3.912023 * jax.random.uniform(streams_of[3], (SLOTS,), jnp.float32) ** block_levels(streams_of[3], (SLOTS,), ((0, 256),), -0.2, 0.2)), 0.002, 0.1)
    weights = with_ends(jax.random.randint(streams_of[4], (SECTORS, SLOTS), 0, 9), jax.random.fold_in(streams_of[4], 1), 0, 8).astype(jnp.int32)
    live_rows = draw_live_rows(jax.random.fold_in(streams_of[6], 71), 0)
    return dict(spectrum=spectrum, quantile_index=quantile_index, bands=bands, default_prob=default_prob, weights=weights, live_rows=live_rows)


def reference(spectrum, quantile_index, bands, default_prob, weights, live_rows):
    loss_field = jnp.fft.ifft(spectrum[0] + 1j * spectrum[1], axis=2).real.astype(jnp.float32)
    suffix = jnp.cumsum(loss_field[:, :, ::-1], axis=2)[:, :, ::-1]
    targets = (quantile_index[:, None] - jnp.arange(1, BANDS + 1, dtype=jnp.int32)[None, :]).astype(jnp.int32)
    tables = jnp.take_along_axis(suffix, jnp.broadcast_to(targets[:, None, :], (SCEN, SECTORS, BANDS)), axis=2)
    slot_index = jnp.arange(SLOTS, dtype=jnp.int32)
    device_index = (slot_index // CAP).astype(jnp.int32)
    live_count = jnp.take(live_rows.reshape(-1), device_index)
    live_mask = (slot_index % CAP) < live_count
    exposure = bands.astype(jnp.float32)
    scaled = jnp.where(live_mask[None, :], weights.astype(jnp.float32) * (default_prob * exposure / 256.0)[None, :], jnp.float32(0.0))
    band_rows = (bands - 1).astype(jnp.int32)

    def one_scenario(table):
        product = scaled * jnp.take(table, band_rows, axis=1)
        return jnp.sum(product, axis=0), jnp.sum(product, axis=1)

    obligor_contrib, sector_sum = lax.map(one_scenario, tables)
    sector_share = sector_sum * (SECTORS / OBLIGORS)
    return (obligor_contrib, sector_share)
```

```python
import math

import jax
import jax.numpy as jnp
from jax import lax
from jax.experimental import pallas as pl
from jax.experimental.pallas import tpu as pltpu
from jax.sharding import PartitionSpec as P

GRID = 65536
BANDS = 1024
OBL_DEV = 1024
LANES = 128
HALF = BANDS // 2
A_LEN = 32
BLOCK = 512
F32 = jnp.float32
BF16 = jnp.bfloat16
I32 = jnp.int32


def iota(shape, dim):
    return lax.broadcasted_iota(I32, shape, dim)


def cos_sin(turns, log_grid):
    quarter_log = log_grid - 2
    quadrant = (turns + (1 << (quarter_log - 1))) >> quarter_log
    rest = turns - (quadrant << quarter_log)
    x = rest.astype(F32) * F32(2.0 * math.pi / (1 << log_grid))
    y = x * x
    sine = x * (1.0 + y * (-1.0 / 6 + y * (1.0 / 120 + y * (-1.0 / 5040 + y * (1.0 / 362880)))))
    cosine = 1.0 + y * (
        -0.5 + y * (1.0 / 24 + y * (-1.0 / 720 + y * (1.0 / 40320 - y * (1.0 / 3628800))))
    )
    odd = (quadrant & 1) == 1
    first = jnp.where(odd, cosine, sine)
    second = jnp.where(odd, sine, cosine)
    return (
        jnp.where(((quadrant + 1) & 2) == 2, -second, second),
        jnp.where((quadrant & 2) == 2, -first, first),
    )


def two_parts(value):
    high = value.astype(BF16).astype(F32)
    return high, value - high


def spectral_kernel(place, quantile, spec, mine, other, lhs, grid, turn_cos, turn_sin, table, offset):
    part = place[0]
    core = place[1]
    scen = spec.shape[1]
    rows = 2 * scen
    shape = (A_LEN, LANES)
    freq = part * (A_LEN * LANES) + iota(shape, 0) * LANES + iota(shape, 1)
    zero = freq == 0
    half_cos, half_sin = cos_sin(freq, 17)
    v_im = jnp.where(zero, 0.0, 0.5 * half_cos / jnp.where(zero, 1.0, half_sin))
    v_re = jnp.where(zero, 0.0, 0.5)
    band_lane = iota((1, LANES), 1)
    for c in range(scen):
        q_less = quantile[c] - 1
        w_cos, w_sin = cos_sin((freq * q_less) & (GRID - 1), 16)
        u_re = v_re * w_cos - v_im * w_sin
        u_im = v_re * w_sin + v_im * w_cos
        for k in range(2):
            x_re = spec[0, c, pl.ds(k, A_LEN, stride=2), :]
            x_im = spec[1, c, pl.ds(k, A_LEN, stride=2), :]
            z_re = x_re * u_re - x_im * u_im
            z_im = x_re * u_im + x_im * u_re
            re_high, re_low = two_parts(z_re)
            im_high, im_low = two_parts(z_im)
            turned = jnp.concatenate([re_high, im_high, re_low, im_low], 0).T.astype(BF16)
            row = k * scen + c
            lhs[row * LANES : (row + 1) * LANES, :LANES] = turned
            lhs[row * LANES : (row + 1) * LANES, LANES:] = turned
            total = jnp.sum(x_re * v_re - x_im * v_im)
            at_zero = jnp.where(part == 0, x_re[0:1, 0:1], 0.0)
            line = at_zero * (GRID - q_less + band_lane).astype(F32) - total
            offset[row : row + 1, :] = line
            offset[rows + row : rows + row + 1, :] = jnp.broadcast_to(at_zero, (1, LANES))
    d_shape = (A_LEN, HALF)
    d_turn = ((part * A_LEN + iota(d_shape, 0)) * iota(d_shape, 1)) & (HALF - 1)
    d_cos, d_sin = cos_sin(d_turn, 9)
    dft = jnp.concatenate(
        [jnp.concatenate([d_cos, -d_sin], 1), jnp.concatenate([d_sin, d_cos], 1)], 0
    )
    d_high, d_low = two_parts(dft)
    d_high = d_high.astype(BF16)
    d_low = d_low.astype(BF16)
    table[...] = jnp.concatenate([d_high, d_high, d_low, d_low], 0)
    t_shape = (LANES, LANES)
    run_cos, run_sin = cos_sin(iota(t_shape, 0) * iota(t_shape, 1), 16)
    step_cos, step_sin = cos_sin(iota(t_shape, 0) * LANES, 16)
    for m in range(8):
        turn_cos[:, m * LANES : (m + 1) * LANES] = run_cos
        turn_sin[:, m * LANES : (m + 1) * LANES] = run_sin
        run_cos, run_sin = (
            run_cos * step_cos - run_sin * step_sin,
            run_sin * step_cos + run_cos * step_sin,
        )
    group = 4
    for g in range(rows // group):
        grid[...] = jnp.dot(
            lhs[g * group * LANES : (g + 1) * group * LANES, :],
            table[...],
            preferred_element_type=F32,
        )

        def tile(t, _):
            lane = pl.multiple_of(t * LANES, LANES)
            for h in range(2):
                acc = [None] * group
                for b in range(LANES // 8):
                    tc = turn_cos[b * 8 : (b + 1) * 8, pl.ds(h * HALF + lane, LANES)]
                    ts = turn_sin[b * 8 : (b + 1) * 8, pl.ds(h * HALF + lane, LANES)]
                    for r in range(group):
                        at = r * LANES + b * 8
                        term = (
                            grid[at : at + 8, pl.ds(lane, LANES)] * tc
                            + grid[at : at + 8, pl.ds(HALF + lane, LANES)] * ts
                        )
                        acc[r] = term if acc[r] is None else acc[r] + term
                for r in range(group):
                    row = g * group + r
                    line = jnp.sum(acc[r], axis=0, keepdims=True)
                    moved = (h * HALF + lane).astype(F32)
                    line = line + offset[row : row + 1, :]
                    line = line + offset[rows + row : rows + row + 1, :] * moved
                    line = line * F32(1.0 / GRID)

                    @pl.when(core == h)
                    def _():
                        mine[pl.ds(t * rows + row, 1), :] = line

                    @pl.when(core != h)
                    def _():
                        other[pl.ds(t * rows + row, 1), :] = line

            return 0

        lax.fori_loop(0, HALF // LANES, tile, 0)


def spectral(place, quantile, spec):
    scen = spec.shape[1]
    rows = 2 * scen
    smem = pl.BlockSpec(memory_space=pltpu.SMEM)
    vmem = pl.BlockSpec(memory_space=pltpu.VMEM)
    out = jax.ShapeDtypeStruct((HALF // LANES * rows, LANES), F32)
    return pl.pallas_call(
        spectral_kernel,
        out_shape=(out, out),
        in_specs=[smem, smem, vmem],
        out_specs=(vmem, vmem),
        scratch_shapes=[
            pltpu.VMEM((rows * LANES, 2 * LANES), BF16),
            pltpu.VMEM((4 * LANES, 2 * HALF), F32),
            pltpu.VMEM((LANES, BANDS), F32),
            pltpu.VMEM((LANES, BANDS), F32),
            pltpu.VMEM((2 * LANES, 2 * HALF), BF16),
            pltpu.VMEM((2 * rows, LANES), F32),
        ],
        cost_estimate=pl.CostEstimate(flops=3_000_000_000, bytes_accessed=600_000, transcendentals=0),
        name="spectral",
    )(place, quantile, spec)


def slot_factor(bands, prob):
    return prob * bands.astype(F32) / 256.0


def band_weights_kernel(live, bands, prob, weights, out, acc):
    sectors = weights.shape[0]
    acc[...] = jnp.zeros_like(acc)

    def block(n, _):
        at = pl.multiple_of(n * BLOCK, BLOCK)
        band = bands[:, pl.ds(at, BLOCK)]
        factor = slot_factor(band, prob[:, pl.ds(at, BLOCK)])
        alive = at + iota((1, BLOCK), 1) < live[0]
        factor = jnp.where(alive, factor, 0.0)
        index = band - 1
        low = index & 255
        high = index >> 8
        value = weights[:, pl.ds(at, BLOCK)].astype(F32) * factor
        v_high, v_low = two_parts(value)
        pieces = []
        for h in range(4):
            here = high == h
            pieces.append(jnp.where(here, v_high, 0.0).astype(BF16))
            pieces.append(jnp.where(here, v_low, 0.0).astype(BF16))
        left = jnp.concatenate(pieces, 0)
        hot = (iota((256, BLOCK), 0) == low).astype(F32).astype(BF16)
        acc[...] += lax.dot_general(
            left, hot, (((1,), (1,)), ((), ())), preferred_element_type=F32
        )
        return 0

    lax.fori_loop(0, (live[0] + BLOCK - 1) // BLOCK, block, 0)
    for h in range(4):
        both = acc[h * 2 * sectors : (h * 2 + 1) * sectors, :] + acc[
            (h * 2 + 1) * sectors : (h * 2 + 2) * sectors, :
        ]
        out[:, 2 * h, :] = both[:, :LANES]
        out[:, 2 * h + 1, :] = both[:, LANES:]


def band_weights(live, bands, prob, weights):
    sectors = weights.shape[0]
    smem = pl.BlockSpec(memory_space=pltpu.SMEM)
    vmem = pl.BlockSpec(memory_space=pltpu.VMEM)
    return pl.pallas_call(
        band_weights_kernel,
        out_shape=jax.ShapeDtypeStruct((sectors, BANDS // LANES, LANES), F32),
        in_specs=[smem, vmem, vmem, vmem],
        out_specs=vmem,
        scratch_shapes=[pltpu.VMEM((8 * sectors, 256), F32)],
        cost_estimate=pl.CostEstimate(flops=600_000_000, bytes_accessed=700_000, transcendentals=0),
        name="band_weights",
    )(live, bands, prob, weights)


def spread_kernel(mine, got, out):
    value = mine[...] + got[...]
    for n in range(out.shape[0]):
        out[n] = value


def spread(mine, got, copies):
    return pl.pallas_call(
        spread_kernel,
        out_shape=jax.ShapeDtypeStruct((copies, *mine.shape), F32),
        name="spread",
    )(mine, got)


def join_kernel(parts, sums, out):
    value = parts[0]
    for n in range(1, parts.shape[0]):
        value = value + parts[n]
    rows = value.shape[0]
    for n in range(out.shape[0]):
        out[n, :rows, :] = value
        out[n, rows:, :] = sums[n]


def join(parts, sums):
    peers, extra, lanes = sums.shape
    return pl.pallas_call(
        join_kernel,
        out_shape=jax.ShapeDtypeStruct((peers, parts.shape[1] + extra, lanes), F32),
        name="join",
    )(parts, sums)


def lookup_kernel(*refs, last):
    if last:
        place, live, tables, bands, prob, weights, before, out, lhs = refs
    else:
        place, live, tables, bands, weights, out, lhs = refs
    peers = tables.shape[0]
    rows = HALF // LANES
    each = 16
    count = peers * each
    sectors = weights.shape[0]
    for t in range(rows):
        value = tables[:, t * each : (t + 1) * each, :].reshape(count, LANES)
        high, low = two_parts(value)
        lhs[:count, t * LANES : (t + 1) * LANES] = high.astype(BF16)
        lhs[count:, t * LANES : (t + 1) * LANES] = low.astype(BF16)
    first = place[1] * HALF if not last else (1 - place[1]) * HALF
    blocks = (live[0] + BLOCK - 1) // BLOCK

    def block(n, _):
        at = pl.multiple_of(n * BLOCK, BLOCK)
        band = bands[:, pl.ds(at, BLOCK)]
        hot = (iota((HALF, BLOCK), 0) == band - 1 - first).astype(F32).astype(BF16)
        found = jnp.dot(lhs[...], hot, preferred_element_type=F32)
        weight = weights[:, pl.ds(at, BLOCK)].astype(F32)
        scen = count // sectors
        acc = jnp.zeros((scen, BLOCK), F32)
        for k in range(sectors):
            entry = found[k * scen : (k + 1) * scen] + found[count + k * scen : count + (k + 1) * scen]
            acc = acc + entry * weight[k : k + 1, :]
        if last:
            factor = slot_factor(band, prob[:, pl.ds(at, BLOCK)])
            alive = at + iota((1, BLOCK), 1) < live[0]
            acc = jnp.where(alive, (acc + before[:, pl.ds(at, BLOCK)]) * factor, 0.0)
        out[:, pl.ds(at, BLOCK)] = acc
        return 0

    lax.fori_loop(0, blocks, block, 0)
    if last:

        def empty(n, _):
            at = pl.multiple_of(n * BLOCK, BLOCK)
            out[:, pl.ds(at, BLOCK)] = jnp.zeros((out.shape[0], BLOCK), F32)
            return 0

        lax.fori_loop(blocks, out.shape[1] // BLOCK, empty, 0)


def lookup(place, live, tables, bands, prob, weights, before):
    import functools

    last = before is not None
    slots = bands.shape[1]
    sectors = weights.shape[0]
    scen = tables.shape[0] * 16 // sectors
    smem = pl.BlockSpec(memory_space=pltpu.SMEM)
    vmem = pl.BlockSpec(memory_space=pltpu.VMEM)
    args = [place, live, tables, bands] + ([prob] if last else []) + [weights] + ([before] if last else [])
    return pl.pallas_call(
        functools.partial(lookup_kernel, last=last),
        out_shape=jax.ShapeDtypeStruct((scen, slots), F32),
        in_specs=[smem, smem] + [vmem] * (len(args) - 2),
        out_specs=vmem,
        scratch_shapes=[pltpu.VMEM((tables.shape[0] * 32, HALF), BF16)],
        cost_estimate=pl.CostEstimate(flops=4_300_000_000, bytes_accessed=1_000_000, transcendentals=0),
        name="lookup_last" if last else "lookup_first",
    )(*args)


def share_kernel(place, near, far, out):
    core = place[1]
    peers = near.shape[0]
    sums = near[0, 64:, :]
    for n in range(1, peers):
        sums = sums + near[n, 64:, :]
    near_rows = near[place[2], :64, :]
    far_rows = far[place[2], :64, :]
    acc = [jnp.zeros((8, LANES), F32) for _ in range(2)]
    for t in range(4):
        for h in range(2):
            block = jnp.where(core == h, near_rows[t * 16 : (t + 1) * 16], far_rows[t * 16 : (t + 1) * 16])
            for k in range(2):
                chunk = h * 4 + t
                acc[k] = acc[k] + block[k * 8 : (k + 1) * 8] * sums[k * 8 + chunk : k * 8 + chunk + 1, :]
    both = jnp.concatenate(acc + [jnp.zeros((LANES - 16, LANES), F32)], 0).T
    line = jnp.sum(both, axis=0, keepdims=True)
    for n in range(out.shape[0]):
        out[n] = line


def share(place, near, far, copies):
    smem = pl.BlockSpec(memory_space=pltpu.SMEM)
    vmem = pl.BlockSpec(memory_space=pltpu.VMEM)
    return pl.pallas_call(
        share_kernel,
        out_shape=jax.ShapeDtypeStruct((copies, 1, LANES), F32),
        in_specs=[smem, vmem, vmem],
        out_specs=vmem,
        name="share",
    )(place, near, far)


def on_device(spectrum, quantile_index, bands, default_prob, weights, live_rows):
    scen, sec_local = spectrum.shape[1], spectrum.shape[2]
    n_obl = lax.axis_size("obl")
    n_sector = lax.axis_size("sector")
    part = lax.axis_index("obl").astype(I32)
    place = jnp.stack([part, part & 1, lax.axis_index("sector").astype(I32)])
    live = live_rows.reshape(1)
    spec = spectrum.reshape(2, scen, sec_local, A_LEN, LANES).transpose(0, 1, 3, 2, 4)
    spec = spec.reshape(2, scen, A_LEN * sec_local, LANES)
    bands = bands[None, :]
    prob = default_prob[None, :]
    swap = [(n, n ^ 1) for n in range(n_obl)]
    same_core = [[n for n in range(n_obl) if n % 2 == c] for c in range(2)]

    mine, other = spectral(place, quantile_index, spec)
    got = lax.ppermute(other, "obl", swap)
    copies = spread(mine, got, n_obl // 2)
    parts = lax.all_to_all(copies, "obl", 0, 0, axis_index_groups=same_core, tiled=True)
    sums = band_weights(live, bands, prob, weights).reshape(n_sector, 16, LANES)
    near = lax.all_to_all(join(parts, sums), "sector", 0, 0, tiled=True)
    far = lax.ppermute(near, "obl", swap)
    before = lookup(place, live, near, bands, prob, weights, None)
    shares = lax.all_to_all(share(place, near, far, n_obl), "obl", 0, 0, tiled=True)
    contrib = lookup(place, live, far, bands, prob, weights, before)
    obligors = OBL_DEV * n_sector * n_obl
    total = jnp.sum(shares, axis=0)[0, : sec_local * scen].reshape(sec_local, scen).T
    return contrib, total * (sec_local * n_sector / obligors)


def solution(mesh):
    in_specs = (
        P(None, None, "sector", "obl"),
        P(),
        P(("sector", "obl")),
        P(("sector", "obl")),
        P(None, ("sector", "obl")),
        P("sector", "obl"),
    )
    out_specs = (P(None, ("sector", "obl")), P(None, "sector"))
    return jax.shard_map(
        on_device, mesh=mesh, in_specs=in_specs, out_specs=out_specs, check_vma=False
    )
```

```python
import functools
import math

import jax
import jax.numpy as jnp
from jax import lax
from jax.experimental import pallas as pl
from jax.experimental.pallas import tpu as pltpu
from jax.sharding import PartitionSpec as P

GRID = 65536
BANDS = 1024
OBL_DEV = 1024
LANES = 128
HALF = BANDS // 2
A_LEN = 32
BLOCK = 512
F32 = jnp.float32
BF16 = jnp.bfloat16
I32 = jnp.int32


def iota(shape, dim):
    return lax.broadcasted_iota(I32, shape, dim)


def cos_sin(turns, log_grid):
    quarter_log = log_grid - 2
    quadrant = (turns + (1 << (quarter_log - 1))) >> quarter_log
    rest = turns - (quadrant << quarter_log)
    x = rest.astype(F32) * F32(2.0 * math.pi / (1 << log_grid))
    y = x * x
    sine = x * (1.0 + y * (-1.0 / 6 + y * (1.0 / 120 + y * (-1.0 / 5040 + y * (1.0 / 362880)))))
    cosine = 1.0 + y * (
        -0.5 + y * (1.0 / 24 + y * (-1.0 / 720 + y * (1.0 / 40320 - y * (1.0 / 3628800))))
    )
    odd = (quadrant & 1) == 1
    first = jnp.where(odd, cosine, sine)
    second = jnp.where(odd, sine, cosine)
    return (
        jnp.where(((quadrant + 1) & 2) == 2, -second, second),
        jnp.where((quadrant & 2) == 2, -first, first),
    )


def two_parts(value):
    high = value.astype(BF16).astype(F32)
    return high, value - high


def spectral_kernel(quantile, spec, mine, other, lhs, turn_cos, turn_sin, table, firsts, sums, lines, *grids):
    part = lax.axis_index("obl").astype(I32)
    core = part & 1
    scen = spec.shape[1]
    rows = 2 * scen
    shape = (A_LEN, LANES)
    freq = part * (A_LEN * LANES) + iota(shape, 0) * LANES + iota(shape, 1)
    zero = freq == 0
    half_cos, half_sin = cos_sin(freq, 17)
    v_im = jnp.where(zero, 0.0, 0.5 * half_cos / jnp.where(zero, 1.0, half_sin))
    v_re = jnp.where(zero, 0.0, 0.5)
    d_shape = (A_LEN, HALF)
    d_turn = ((part * A_LEN + iota(d_shape, 0)) * iota(d_shape, 1)) & (HALF - 1)
    d_cos, d_sin = cos_sin(d_turn, 9)
    dft = jnp.concatenate(
        [jnp.concatenate([d_cos, -d_sin], 1), jnp.concatenate([d_sin, d_cos], 1)], 0
    )
    d_high, d_low = two_parts(dft)
    d_high = d_high.astype(BF16)
    d_low = d_low.astype(BF16)
    table[...] = jnp.concatenate([d_high, d_high, d_low, d_low], 0)
    for c in range(scen):
        w_cos, w_sin = cos_sin((freq * (quantile[c] - 1)) & (GRID - 1), 16)
        u_re = v_re * w_cos - v_im * w_sin
        u_im = v_re * w_sin + v_im * w_cos
        for k in range(2):
            x_re = spec[0, c, pl.ds(k, A_LEN, stride=2), :]
            x_im = spec[1, c, pl.ds(k, A_LEN, stride=2), :]
            z_re = x_re * u_re - x_im * u_im
            z_im = x_re * u_im + x_im * u_re
            re_high, re_low = two_parts(z_re)
            im_high, im_low = two_parts(z_im)
            turned = jnp.concatenate([re_high, im_high, re_low, im_low], 0).T.astype(BF16)
            row = k * scen + c
            lhs[row * LANES : (row + 1) * LANES, :LANES] = turned
            lhs[row * LANES : (row + 1) * LANES, LANES:] = turned
            sums[row : row + 1, :] = jnp.sum(x_re * v_re - x_im * v_im, axis=0, keepdims=True)
            firsts[row : row + 1, :] = x_re[0:1, :]
    t_shape = (LANES, LANES)
    run_cos, run_sin = cos_sin(iota(t_shape, 0) * iota(t_shape, 1), 16)
    step_cos, step_sin = cos_sin(iota(t_shape, 0) * LANES, 16)
    for m in range(8):
        turn_cos[:, m * LANES : (m + 1) * LANES] = run_cos
        turn_sin[:, m * LANES : (m + 1) * LANES] = run_sin
        run_cos, run_sin = (
            run_cos * step_cos - run_sin * step_sin,
            run_sin * step_cos + run_cos * step_sin,
        )
    group = rows // len(grids)
    tiles = HALF // LANES
    for g, grid in enumerate(grids):
        grid[...] = jnp.dot(
            lhs[g * group * LANES : (g + 1) * group * LANES, :],
            table[...],
            preferred_element_type=F32,
        )
        for t in range(tiles):
            lane = t * LANES
            acc = [[None] * group for _ in range(2)]
            for b in range(LANES // 8):
                turn = [
                    (
                        turn_cos[b * 8 : (b + 1) * 8, h * HALF + lane : h * HALF + lane + LANES],
                        turn_sin[b * 8 : (b + 1) * 8, h * HALF + lane : h * HALF + lane + LANES],
                    )
                    for h in range(2)
                ]
                for r in range(group):
                    at = r * LANES + b * 8
                    g_re = grid[at : at + 8, lane : lane + LANES]
                    g_im = grid[at : at + 8, HALF + lane : HALF + lane + LANES]
                    for h in range(2):
                        term = g_re * turn[h][0] + g_im * turn[h][1]
                        acc[h][r] = term if acc[h][r] is None else acc[h][r] + term
            for h in range(2):
                for r in range(group):
                    at = ((h * tiles + t) * rows + g * group + r) * 8
                    lines[at : at + 8, :] = acc[h][r]
    total = jnp.sum(sums[...], axis=1, keepdims=True)
    at_zero = jnp.where(part == 0, firsts[:, 0:1], 0.0)
    lane_at = iota((1, LANES), 1)
    c_of = iota((scen, 1), 0)
    q_less = jnp.zeros((scen, 1), I32)
    for c in range(scen):
        q_less = jnp.where(c_of == c, quantile[c] - 1, q_less)
    for h in range(2):
        for t in range(tiles):
            for k in range(2):
                base = ((h * tiles + t) * rows + k * scen) * 8
                value = lines[pl.ds(base, scen, stride=8), :]
                for s in range(1, 8):
                    value = value + lines[pl.ds(base + s, scen, stride=8), :]
                size = (GRID - q_less + (h * HALF + t * LANES + lane_at)).astype(F32)
                here = slice(k * scen, (k + 1) * scen)
                value = (value + at_zero[here] * size - total[here]) * F32(1.0 / GRID)
                lines[pl.ds(base, scen), :] = value

    def send(h, to):
        for t in range(tiles):
            for k in range(2):
                base = ((h * tiles + t) * rows + k * scen) * 8
                to[t * rows + k * scen : t * rows + (k + 1) * scen, :] = lines[base : base + scen, :]

    @pl.when(core == 0)
    def _():
        send(0, mine)
        send(1, other)

    @pl.when(core == 1)
    def _():
        send(1, mine)
        send(0, other)


def spectral(quantile, spec):
    scen = spec.shape[1]
    rows = 2 * scen
    groups = 4
    smem = pl.BlockSpec(memory_space=pltpu.SMEM)
    vmem = pl.BlockSpec(memory_space=pltpu.VMEM)
    out = jax.ShapeDtypeStruct((HALF // LANES * rows, LANES), F32)
    return pl.pallas_call(
        spectral_kernel,
        out_shape=(out, out),
        in_specs=[smem, vmem],
        out_specs=(vmem, vmem),
        scratch_shapes=[
            pltpu.VMEM((rows * LANES, 2 * LANES), BF16),
            pltpu.VMEM((LANES, BANDS), F32),
            pltpu.VMEM((LANES, BANDS), F32),
            pltpu.VMEM((2 * LANES, 2 * HALF), BF16),
            pltpu.VMEM((rows, LANES), F32),
            pltpu.VMEM((rows, LANES), F32),
            pltpu.VMEM((BANDS // LANES * rows * 8, LANES), F32),
        ]
        + [pltpu.VMEM((rows // groups * LANES, 2 * HALF), F32)] * groups,
        compiler_params=pltpu.CompilerParams(vmem_limit_bytes=24 << 20),
        cost_estimate=pl.CostEstimate(flops=3_000_000_000, bytes_accessed=600_000, transcendentals=0),
        name="spectral",
    )(quantile, spec)


def slot_factor(bands, prob):
    return prob * bands.astype(F32) / 256.0


def band_weights_kernel(live, bands, prob, weights, mine, other, acc):
    sectors = weights.shape[0]
    acc[...] = jnp.zeros_like(acc)

    def block(n, _):
        at = pl.multiple_of(n * BLOCK, BLOCK)
        band = bands[:, pl.ds(at, BLOCK)]
        factor = slot_factor(band, prob[:, pl.ds(at, BLOCK)])
        alive = at + iota((1, BLOCK), 1) < live[0]
        factor = jnp.where(alive, factor, 0.0)
        index = band - 1
        low = index & 255
        high = index >> 8
        value = weights[:, pl.ds(at, BLOCK)].astype(F32) * factor
        v_high, v_low = two_parts(value)
        pieces = []
        for h in range(4):
            here = high == h
            pieces.append(jnp.where(here, v_high, 0.0).astype(BF16))
            pieces.append(jnp.where(here, v_low, 0.0).astype(BF16))
        left = jnp.concatenate(pieces, 0)
        hot = (iota((256, BLOCK), 0) == low).astype(F32).astype(BF16)
        acc[...] += lax.dot_general(
            left, hot, (((1,), (1,)), ((), ())), preferred_element_type=F32
        )
        return 0

    lax.fori_loop(0, (live[0] + BLOCK - 1) // BLOCK, block, 0)
    core = lax.axis_index("obl").astype(I32) & 1

    def send(half, to):
        for h in range(2):
            at = (2 * half + h) * 2 * sectors
            both = acc[at : at + sectors, :] + acc[at + sectors : at + 2 * sectors, :]
            for m in range(2):
                chunk = both[:, m * LANES : (m + 1) * LANES]
                to[pl.ds(2 * h + m, sectors, stride=4), :] = chunk

    @pl.when(core == 0)
    def _():
        send(0, mine)
        send(1, other)

    @pl.when(core == 1)
    def _():
        send(1, mine)
        send(0, other)


def band_weights(live, bands, prob, weights):
    sectors = weights.shape[0]
    smem = pl.BlockSpec(memory_space=pltpu.SMEM)
    vmem = pl.BlockSpec(memory_space=pltpu.VMEM)
    out = jax.ShapeDtypeStruct((sectors * HALF // LANES, LANES), F32)
    return pl.pallas_call(
        band_weights_kernel,
        out_shape=(out, out),
        in_specs=[smem, vmem, vmem, vmem],
        out_specs=(vmem, vmem),
        scratch_shapes=[pltpu.VMEM((8 * sectors, 256), F32)],
        compiler_params=pltpu.CompilerParams(vmem_limit_bytes=12 << 20),
        cost_estimate=pl.CostEstimate(flops=600_000_000, bytes_accessed=700_000, transcendentals=0),
        name="band_weights",
    )(live, bands, prob, weights)


def spread_kernel(mine, got, out):
    value = mine[...] + got[...]
    for n in range(out.shape[0]):
        out[n] = value


def spread(mine, got, copies):
    return pl.pallas_call(
        spread_kernel,
        out_shape=jax.ShapeDtypeStruct((copies, *mine.shape), F32),
        compiler_params=pltpu.CompilerParams(vmem_limit_bytes=4 << 20),
        name="spread",
    )(mine, got)


def join_kernel(parts, sums, got, out, own):
    value = parts[0]
    for n in range(1, parts.shape[0]):
        value = value + parts[n]
    rows = value.shape[0]
    own[...] = value
    for n in range(out.shape[0]):
        out[n, :rows, :] = value
        out[n, rows:, :] = sums[n] + got[n]


def join(parts, sums, got):
    peers, extra, lanes = sums.shape
    rows = parts.shape[1]
    return pl.pallas_call(
        join_kernel,
        out_shape=(
            jax.ShapeDtypeStruct((peers, rows + extra, lanes), F32),
            jax.ShapeDtypeStruct((rows, lanes), F32),
        ),
        compiler_params=pltpu.CompilerParams(vmem_limit_bytes=4 << 20),
        name="join",
    )(parts, sums, got)


def lookup_kernel(*refs, last):
    if last:
        live, tables, bands, prob, weights, before, out, lhs = refs
    else:
        live, tables, bands, weights, out, lhs = refs
    core = lax.axis_index("obl").astype(I32) & 1
    peers = tables.shape[0]
    rows = HALF // LANES
    each = 16
    count = peers * each
    sectors = weights.shape[0]
    scen = count // sectors
    for t in range(rows):
        value = tables[:, t * each : (t + 1) * each, :].reshape(count, LANES)
        high, low = two_parts(value)
        lhs[:count, t * LANES : (t + 1) * LANES] = high.astype(BF16)
        lhs[count:, t * LANES : (t + 1) * LANES] = low.astype(BF16)
    first = (core if not last else 1 - core) * HALF
    step = 2 * BLOCK
    steps = (live[0] + step - 1) // step

    def block(n, _):
        for part in range(2):
            at = pl.multiple_of(n * step + part * BLOCK, BLOCK)
            band = bands[:, pl.ds(at, BLOCK)]
            hot = (iota((HALF, BLOCK), 0) == band - 1 - first).astype(F32).astype(BF16)
            found = jnp.dot(lhs[...], hot, preferred_element_type=F32)
            weight = weights[:, pl.ds(at, BLOCK)].astype(F32)
            acc = jnp.zeros((scen, BLOCK), F32)
            for k in range(sectors):
                entry = found[k * scen : (k + 1) * scen] + found[count + k * scen : count + (k + 1) * scen]
                acc = acc + entry * weight[k : k + 1, :]
            if last:
                factor = slot_factor(band, prob[:, pl.ds(at, BLOCK)])
                alive = at + iota((1, BLOCK), 1) < live[0]
                acc = jnp.where(alive, (acc + before[:, pl.ds(at, BLOCK)]) * factor, 0.0)
            out[:, pl.ds(at, BLOCK)] = acc
        return 0

    lax.fori_loop(0, steps, block, 0)
    if last:

        def empty(n, _):
            at = pl.multiple_of(n * step, step)
            out[:, pl.ds(at, step)] = jnp.zeros((out.shape[0], step), F32)
            return 0

        lax.fori_loop(steps, out.shape[1] // step, empty, 0)


def lookup(live, tables, bands, prob, weights, before):
    last = before is not None
    slots = bands.shape[1]
    sectors = weights.shape[0]
    scen = tables.shape[0] * 16 // sectors
    smem = pl.BlockSpec(memory_space=pltpu.SMEM)
    vmem = pl.BlockSpec(memory_space=pltpu.VMEM)
    args = [live, tables, bands] + ([prob] if last else []) + [weights] + ([before] if last else [])
    return pl.pallas_call(
        functools.partial(lookup_kernel, last=last),
        out_shape=jax.ShapeDtypeStruct((scen, slots), F32),
        in_specs=[smem] + [vmem] * (len(args) - 1),
        out_specs=vmem,
        scratch_shapes=[pltpu.VMEM((tables.shape[0] * 32, HALF), BF16)],
        compiler_params=pltpu.CompilerParams(vmem_limit_bytes=24 << 20),
        cost_estimate=pl.CostEstimate(flops=4_300_000_000, bytes_accessed=1_000_000, transcendentals=0),
        name="lookup_last" if last else "lookup_first",
    )(*args)


def share_kernel(own, near, out):
    rows = own.shape[0]
    sums = near[0, rows:, :]
    for n in range(1, near.shape[0]):
        sums = sums + near[n, rows:, :]
    acc = [jnp.zeros((8, LANES), F32) for _ in range(2)]
    for t in range(4):
        for k in range(2):
            at = t * 16 + k * 8
            acc[k] = acc[k] + own[at : at + 8, :] * sums[k * 4 + t : k * 4 + t + 1, :]
    both = jnp.concatenate(acc + [jnp.zeros((LANES - 16, LANES), F32)], 0).T
    line = jnp.sum(both, axis=0, keepdims=True)
    for n in range(out.shape[0]):
        out[n] = line


def share(own, near, copies):
    return pl.pallas_call(
        share_kernel,
        out_shape=jax.ShapeDtypeStruct((copies, 1, LANES), F32),
        compiler_params=pltpu.CompilerParams(vmem_limit_bytes=4 << 20),
        cost_estimate=pl.CostEstimate(flops=1_000_000, bytes_accessed=100_000, transcendentals=0),
        name="share",
    )(own, near)


def total_kernel(shares, out, *, scale):
    line = shares[0]
    for n in range(1, shares.shape[0]):
        line = line + shares[n]
    line = line * F32(scale)
    out[0:1, :] = line[:, :8]
    out[1:2, :] = line[:, 8:16]


def total_of(shares, scale):
    return pl.pallas_call(
        functools.partial(total_kernel, scale=scale),
        out_shape=jax.ShapeDtypeStruct((2, 8), F32),
        compiler_params=pltpu.CompilerParams(vmem_limit_bytes=4 << 20),
        name="total",
    )(shares)


def on_device(spectrum, quantile_index, bands, default_prob, weights, live_rows):
    scen, sec_local = spectrum.shape[1], spectrum.shape[2]
    n_obl = lax.axis_size("obl")
    n_sector = lax.axis_size("sector")
    live = live_rows.reshape(1)
    spec = spectrum.reshape(2, scen, sec_local, A_LEN, LANES).transpose(0, 1, 3, 2, 4)
    spec = spec.reshape(2, scen, A_LEN * sec_local, LANES)
    bands = bands[None, :]
    prob = default_prob[None, :]
    swap = [(n, n ^ 1) for n in range(n_obl)]
    same_core = [[n for n in range(n_obl) if n % 2 == c] for c in range(2)]

    mine, other = spectral(quantile_index, spec)
    got = lax.ppermute(other, "obl", swap)
    copies = spread(mine, got, n_obl // 2)
    parts = lax.all_to_all(copies, "obl", 0, 0, axis_index_groups=same_core, tiled=True)
    sums, other_sums = band_weights(live, bands, prob, weights)
    got_sums = lax.ppermute(other_sums, "obl", swap)
    each = (n_sector, sums.shape[0] // n_sector, LANES)
    joined, own = join(parts, sums.reshape(each), got_sums.reshape(each))
    near = lax.all_to_all(joined, "sector", 0, 0, tiled=True)
    far = lax.ppermute(near, "obl", swap)
    shares = lax.all_to_all(share(own, near, n_obl), "obl", 0, 0, tiled=True)
    before = lookup(live, near, bands, prob, weights, None)
    contrib = lookup(live, far, bands, prob, weights, before)
    total = total_of(shares, sec_local * n_sector / (OBL_DEV * n_sector * n_obl)).T
    return contrib, total


def solution(mesh):
    in_specs = (
        P(None, None, "sector", "obl"),
        P(),
        P(("sector", "obl")),
        P(("sector", "obl")),
        P(None, ("sector", "obl")),
        P("sector", "obl"),
    )
    out_specs = (P(None, ("sector", "obl")), P(None, "sector"))
    return jax.shard_map(
        on_device, mesh=mesh, in_specs=in_specs, out_specs=out_specs, check_vma=False
    )
```

```python
import functools
import math

import jax
import jax.numpy as jnp
from jax import lax
from jax.experimental import pallas as pl
from jax.experimental.pallas import tpu as pltpu
from jax.sharding import PartitionSpec as P


GRID = 65536
BANDS = 1024
OBL_DEV = 1024
LANES = 128
HALF = BANDS // 2
A_LEN = 32
BLOCK = 512
F32 = jnp.float32
BF16 = jnp.bfloat16
I32 = jnp.int32


def iota(shape, dim):
    return lax.broadcasted_iota(I32, shape, dim)


def cos_sin(turns, log_grid):
    quarter_log = log_grid - 2
    quadrant = (turns + (1 << (quarter_log - 1))) >> quarter_log
    rest = turns - (quadrant << quarter_log)
    x = rest.astype(F32) * F32(2.0 * math.pi / (1 << log_grid))
    y = x * x
    sine = x * (1.0 + y * (-1.0 / 6 + y * (1.0 / 120 + y * (-1.0 / 5040 + y * (1.0 / 362880)))))
    cosine = 1.0 + y * (
        -0.5 + y * (1.0 / 24 + y * (-1.0 / 720 + y * (1.0 / 40320 - y * (1.0 / 3628800))))
    )
    odd = (quadrant & 1) == 1
    first = jnp.where(odd, cosine, sine)
    second = jnp.where(odd, sine, cosine)
    return (
        jnp.where(((quadrant + 1) & 2) == 2, -second, second),
        jnp.where((quadrant & 2) == 2, -first, first),
    )


def two_parts(value):
    high = value.astype(BF16).astype(F32)
    return high, value - high


def spectral_kernel(quantile_hbm, spec_hbm, mine, other, quantile, spec, sems, lhs, turn_cos, turn_sin, table, firsts, sums, lines, *grids):
    part = lax.axis_index("obl").astype(I32)
    core = part & 1
    scen = spec.shape[1]
    rows = 2 * scen
    copies = [
        pltpu.make_async_copy(quantile_hbm, quantile, sems.at[0]),
        pltpu.make_async_copy(spec_hbm, spec, sems.at[1]),
    ]
    for copy in copies:
        copy.start()
    shape = (A_LEN, LANES)
    freq = part * (A_LEN * LANES) + iota(shape, 0) * LANES + iota(shape, 1)
    zero = freq == 0
    half_cos, half_sin = cos_sin(freq, 17)
    v_im = jnp.where(zero, 0.0, 0.5 * half_cos / jnp.where(zero, 1.0, half_sin))
    v_re = jnp.where(zero, 0.0, 0.5)
    d_shape = (A_LEN, HALF)
    d_turn = ((part * A_LEN + iota(d_shape, 0)) * iota(d_shape, 1)) & (HALF - 1)
    d_cos, d_sin = cos_sin(d_turn, 9)
    dft = jnp.concatenate(
        [jnp.concatenate([d_cos, -d_sin], 1), jnp.concatenate([d_sin, d_cos], 1)], 0
    )
    d_high, d_low = two_parts(dft)
    d_high = d_high.astype(BF16)
    d_low = d_low.astype(BF16)
    table[...] = jnp.concatenate([d_high, d_high, d_low, d_low], 0)
    t_shape = (LANES, LANES)
    run_cos, run_sin = cos_sin(iota(t_shape, 0) * iota(t_shape, 1), 16)
    step_cos, step_sin = cos_sin(iota(t_shape, 0) * LANES, 16)
    for m in range(8):
        turn_cos[:, m * LANES : (m + 1) * LANES] = run_cos
        turn_sin[:, m * LANES : (m + 1) * LANES] = run_sin
        run_cos, run_sin = (
            run_cos * step_cos - run_sin * step_sin,
            run_sin * step_cos + run_cos * step_sin,
        )
    for copy in copies:
        copy.wait()
    for c in range(scen):
        w_cos, w_sin = cos_sin((freq * (quantile[c] - 1)) & (GRID - 1), 16)
        u_re = v_re * w_cos - v_im * w_sin
        u_im = v_re * w_sin + v_im * w_cos
        for k in range(2):
            x_re = spec[0, c, pl.ds(k, A_LEN, stride=2), :]
            x_im = spec[1, c, pl.ds(k, A_LEN, stride=2), :]
            z_re = x_re * u_re - x_im * u_im
            z_im = x_re * u_im + x_im * u_re
            re_high, re_low = two_parts(z_re)
            im_high, im_low = two_parts(z_im)
            turned = jnp.concatenate([re_high, im_high, re_low, im_low], 0).T.astype(BF16)
            row = k * scen + c
            lhs[row * LANES : (row + 1) * LANES, :LANES] = turned
            lhs[row * LANES : (row + 1) * LANES, LANES:] = turned
            sums[row : row + 1, :] = jnp.sum(x_re * v_re - x_im * v_im, axis=0, keepdims=True)
            firsts[row : row + 1, :] = x_re[0:1, :]
    group = rows // len(grids)
    tiles = HALF // LANES
    for g, grid in enumerate(grids):
        grid[...] = jnp.dot(
            lhs[g * group * LANES : (g + 1) * group * LANES, :],
            table[...],
            preferred_element_type=F32,
        )
        for t in range(tiles):
            lane = t * LANES
            acc = [[None] * group for _ in range(2)]
            for b in range(LANES // 8):
                turn = [
                    (
                        turn_cos[b * 8 : (b + 1) * 8, h * HALF + lane : h * HALF + lane + LANES],
                        turn_sin[b * 8 : (b + 1) * 8, h * HALF + lane : h * HALF + lane + LANES],
                    )
                    for h in range(2)
                ]
                for r in range(group):
                    at = r * LANES + b * 8
                    g_re = grid[at : at + 8, lane : lane + LANES]
                    g_im = grid[at : at + 8, HALF + lane : HALF + lane + LANES]
                    for h in range(2):
                        term = g_re * turn[h][0] + g_im * turn[h][1]
                        acc[h][r] = term if acc[h][r] is None else acc[h][r] + term
            for h in range(2):
                for r in range(group):
                    at = ((h * tiles + t) * rows + g * group + r) * 8
                    lines[at : at + 8, :] = acc[h][r]
    total = jnp.sum(sums[...], axis=1, keepdims=True)
    at_zero = jnp.where(part == 0, firsts[:, 0:1], 0.0)
    lane_at = iota((1, LANES), 1)
    c_of = iota((scen, 1), 0)
    q_less = jnp.zeros((scen, 1), I32)
    for c in range(scen):
        q_less = jnp.where(c_of == c, quantile[c] - 1, q_less)
    for h in range(2):
        for t in range(tiles):
            for k in range(2):
                base = ((h * tiles + t) * rows + k * scen) * 8
                value = lines[pl.ds(base, scen, stride=8), :]
                for s in range(1, 8):
                    value = value + lines[pl.ds(base + s, scen, stride=8), :]
                size = (GRID - q_less + (h * HALF + t * LANES + lane_at)).astype(F32)
                here = slice(k * scen, (k + 1) * scen)
                value = (value + at_zero[here] * size - total[here]) * F32(1.0 / GRID)
                lines[pl.ds(base, scen), :] = value

    def send(h, to):
        for t in range(tiles):
            for k in range(2):
                base = ((h * tiles + t) * rows + k * scen) * 8
                to[t * rows + k * scen : t * rows + (k + 1) * scen, :] = lines[base : base + scen, :]

    @pl.when(core == 0)
    def _():
        send(0, mine)
        send(1, other)

    @pl.when(core == 1)
    def _():
        send(1, mine)
        send(0, other)


def spectral(quantile, spec):
    scen = spec.shape[1]
    rows = 2 * scen
    groups = 4
    hbm = pl.BlockSpec(memory_space=pltpu.HBM)
    vmem = pl.BlockSpec(memory_space=pltpu.VMEM)
    out = jax.ShapeDtypeStruct((HALF // LANES * rows, LANES), F32)
    return pl.pallas_call(
        spectral_kernel,
        out_shape=(out, out),
        in_specs=[hbm, hbm],
        out_specs=(vmem, vmem),
        scratch_shapes=[
            pltpu.SMEM(quantile.shape, I32),
            pltpu.VMEM(spec.shape, F32),
            pltpu.SemaphoreType.DMA((2,)),
            pltpu.VMEM((rows * LANES, 2 * LANES), BF16),
            pltpu.VMEM((LANES, BANDS), F32),
            pltpu.VMEM((LANES, BANDS), F32),
            pltpu.VMEM((2 * LANES, 2 * HALF), BF16),
            pltpu.VMEM((rows, LANES), F32),
            pltpu.VMEM((rows, LANES), F32),
            pltpu.VMEM((BANDS // LANES * rows * 8, LANES), F32),
        ]
        + [pltpu.VMEM((rows // groups * LANES, 2 * HALF), F32)] * groups,
        compiler_params=pltpu.CompilerParams(vmem_limit_bytes=24 << 20),
        cost_estimate=pl.CostEstimate(flops=3_000_000_000, bytes_accessed=600_000, transcendentals=0),
        name="spectral",
    )(
        pltpu.with_memory_space_constraint(quantile, pltpu.HBM),
        pltpu.with_memory_space_constraint(spec, pltpu.HBM),
    )


def slot_factor(bands, prob):
    return prob * bands.astype(F32) / 256.0


def band_weights_kernel(live, bands, prob, weights, mine, other, acc):
    sectors = weights.shape[0]
    acc[...] = jnp.zeros_like(acc)

    def block(n, _):
        at = pl.multiple_of(n * BLOCK, BLOCK)
        band = bands[:, pl.ds(at, BLOCK)]
        factor = slot_factor(band, prob[:, pl.ds(at, BLOCK)])
        alive = at + iota((1, BLOCK), 1) < live[0, 0]
        factor = jnp.where(alive, factor, 0.0)
        index = band - 1
        low = index & 255
        high = index >> 8
        value = weights[:, pl.ds(at, BLOCK)].astype(F32) * factor
        v_high, v_low = two_parts(value)
        pieces = []
        for h in range(4):
            here = high == h
            pieces.append(jnp.where(here, v_high, 0.0).astype(BF16))
            pieces.append(jnp.where(here, v_low, 0.0).astype(BF16))
        left = jnp.concatenate(pieces, 0)
        hot = (iota((256, BLOCK), 0) == low).astype(F32).astype(BF16)
        acc[...] += lax.dot_general(
            left, hot, (((1,), (1,)), ((), ())), preferred_element_type=F32
        )
        return 0

    lax.fori_loop(0, (live[0, 0] + BLOCK - 1) // BLOCK, block, 0)
    core = lax.axis_index("obl").astype(I32) & 1

    def send(half, to):
        for h in range(2):
            at = (2 * half + h) * 2 * sectors
            both = acc[at : at + sectors, :] + acc[at + sectors : at + 2 * sectors, :]
            for m in range(2):
                chunk = both[:, m * LANES : (m + 1) * LANES]
                to[pl.ds(2 * h + m, sectors, stride=4), :] = chunk

    @pl.when(core == 0)
    def _():
        send(0, mine)
        send(1, other)

    @pl.when(core == 1)
    def _():
        send(1, mine)
        send(0, other)


def band_weights(live, bands, prob, weights):
    sectors = weights.shape[0]
    smem = pl.BlockSpec(memory_space=pltpu.SMEM)
    vmem = pl.BlockSpec(memory_space=pltpu.VMEM)
    out = jax.ShapeDtypeStruct((sectors * HALF // LANES, LANES), F32)
    return pl.pallas_call(
        band_weights_kernel,
        out_shape=(out, out),
        in_specs=[smem, vmem, vmem, vmem],
        out_specs=(vmem, vmem),
        scratch_shapes=[pltpu.VMEM((8 * sectors, 256), F32)],
        compiler_params=pltpu.CompilerParams(vmem_limit_bytes=12 << 20),
        cost_estimate=pl.CostEstimate(flops=600_000_000, bytes_accessed=700_000, transcendentals=0),
        name="band_weights",
    )(live, bands, prob, weights)


def spread_kernel(mine, got, out, *, parities):
    value = mine[...] + got[...]
    rows = out.shape[1]
    for n, parity in enumerate(parities):
        out[n] = value[parity * rows : (parity + 1) * rows]


def spread(mine, got, parities):
    return pl.pallas_call(
        functools.partial(spread_kernel, parities=parities),
        out_shape=jax.ShapeDtypeStruct((len(parities), mine.shape[0] // 2, LANES), F32),
        compiler_params=pltpu.CompilerParams(vmem_limit_bytes=4 << 20),
        name="spread",
    )(mine, got)


def join_kernel(parts, sums, got, out, own):
    value = parts[0]
    for n in range(1, parts.shape[0]):
        value = value + parts[n]
    rows = value.shape[0]
    own[...] = value
    for n in range(out.shape[0]):
        out[n, :rows, :] = value
        out[n, rows:, :] = sums[n] + got[n]


def join(parts, sums, got):
    peers, extra, lanes = sums.shape
    rows = parts.shape[1]
    return pl.pallas_call(
        join_kernel,
        out_shape=(
            jax.ShapeDtypeStruct((peers, rows + extra, lanes), F32),
            jax.ShapeDtypeStruct((rows, lanes), F32),
        ),
        compiler_params=pltpu.CompilerParams(vmem_limit_bytes=4 << 20),
        name="join",
    )(parts, sums, got)


def lookup_kernel(*refs, last):
    if last:
        live, same, cross, bands, prob, weights, before, out, lhs = refs
    else:
        live, same, cross, bands, weights, out, lhs = refs
    place = lax.axis_index("obl").astype(I32)
    core = place & 1
    parity = (place >> 1) & 1
    peers = same.shape[0]
    rows = HALF // LANES
    each = 16
    count = peers * each
    sectors = weights.shape[0]
    scen = count // sectors
    for t in range(rows):
        side = same if t < 2 else cross
        at = (t % 2) * each
        value = side[:, at : at + each, :].reshape(count, LANES)
        high, low = two_parts(value)
        lhs[:count, t * LANES : (t + 1) * LANES] = high.astype(BF16)
        lhs[count:, t * LANES : (t + 1) * LANES] = low.astype(BF16)
    want = 1 - parity if last else parity
    step = 2 * BLOCK
    steps = (live[0, 0] + step - 1) // step

    def block(n, _):
        for part in range(2):
            at = pl.multiple_of(n * step + part * BLOCK, BLOCK)
            band = bands[:, pl.ds(at, BLOCK)]
            index = band - 1
            column = (index & 255) + jnp.where((index >> 9) == core, 0, 256)
            column = jnp.where(((index >> 8) & 1) == want, column, -1)
            hot = (iota((HALF, BLOCK), 0) == column).astype(F32).astype(BF16)
            found = jnp.dot(lhs[...], hot, preferred_element_type=F32)
            weight = weights[:, pl.ds(at, BLOCK)].astype(F32)
            acc = jnp.zeros((scen, BLOCK), F32)
            for k in range(sectors):
                entry = found[k * scen : (k + 1) * scen] + found[count + k * scen : count + (k + 1) * scen]
                acc = acc + entry * weight[k : k + 1, :]
            if last:
                factor = slot_factor(band, prob[:, pl.ds(at, BLOCK)])
                alive = at + iota((1, BLOCK), 1) < live[0, 0]
                acc = jnp.where(alive, (acc + before[:, pl.ds(at, BLOCK)]) * factor, 0.0)
            out[:, pl.ds(at, BLOCK)] = acc
        return 0

    lax.fori_loop(0, steps, block, 0)
    if last:

        def empty(n, _):
            at = pl.multiple_of(n * step, step)
            out[:, pl.ds(at, step)] = jnp.zeros((out.shape[0], step), F32)
            return 0

        lax.fori_loop(steps, out.shape[1] // step, empty, 0)


def lookup(live, same, cross, bands, prob, weights, before):
    last = before is not None
    slots = bands.shape[1]
    sectors = weights.shape[0]
    scen = same.shape[0] * 16 // sectors
    smem = pl.BlockSpec(memory_space=pltpu.SMEM)
    vmem = pl.BlockSpec(memory_space=pltpu.VMEM)
    args = [live, same, cross, bands] + ([prob] if last else []) + [weights] + ([before] if last else [])
    return pl.pallas_call(
        functools.partial(lookup_kernel, last=last),
        out_shape=jax.ShapeDtypeStruct((scen, slots), F32),
        in_specs=[smem] + [vmem] * (len(args) - 1),
        out_specs=vmem,
        scratch_shapes=[pltpu.VMEM((same.shape[0] * 32, HALF), BF16)],
        compiler_params=pltpu.CompilerParams(vmem_limit_bytes=24 << 20),
        cost_estimate=pl.CostEstimate(flops=4_300_000_000, bytes_accessed=1_000_000, transcendentals=0),
        name="lookup_last" if last else "lookup_first",
    )(*args)


def share_kernel(own, across, near, out):
    parity = (lax.axis_index("obl").astype(I32) >> 1) & 1
    rows = own.shape[0]
    sums = near[0, rows:, :]
    for n in range(1, near.shape[0]):
        sums = sums + near[n, rows:, :]
    acc = [jnp.zeros((8, LANES), F32) for _ in range(2)]
    for t in range(2):
        for k in range(2):
            at = t * 16 + k * 8
            low = sums[k * 4 + t : k * 4 + t + 1, :]
            high = sums[k * 4 + 2 + t : k * 4 + 3 + t, :]
            acc[k] = acc[k] + own[at : at + 8, :] * jnp.where(parity == 0, low, high)
            acc[k] = acc[k] + across[at : at + 8, :] * jnp.where(parity == 0, high, low)
    both = jnp.concatenate(acc + [jnp.zeros((LANES - 16, LANES), F32)], 0).T
    line = jnp.sum(both, axis=0, keepdims=True)
    for n in range(out.shape[0]):
        out[n] = line


def share(own, across, near, copies):
    return pl.pallas_call(
        share_kernel,
        out_shape=jax.ShapeDtypeStruct((copies, 1, LANES), F32),
        compiler_params=pltpu.CompilerParams(vmem_limit_bytes=4 << 20),
        cost_estimate=pl.CostEstimate(flops=1_000_000, bytes_accessed=100_000, transcendentals=0),
        name="share",
    )(own, across, near)


def total_kernel(shares, out, *, scale):
    line = shares[0]
    for n in range(1, shares.shape[0]):
        line = line + shares[n]
    line = line * F32(scale)
    out[0:1, :] = line[:, :8]
    out[1:2, :] = line[:, 8:16]


def total_of(shares, scale):
    return pl.pallas_call(
        functools.partial(total_kernel, scale=scale),
        out_shape=jax.ShapeDtypeStruct((2, 8), F32),
        compiler_params=pltpu.CompilerParams(vmem_limit_bytes=4 << 20),
        name="total",
    )(shares)


def contributions(spectrum, quantile_index, bands, default_prob, weights, live_rows):
    scen, sec_local = spectrum.shape[1], spectrum.shape[2]
    n_obl = lax.axis_size("obl")
    n_sector = lax.axis_size("sector")
    live = live_rows
    spec = spectrum.reshape(2, scen, sec_local, A_LEN, LANES).transpose(0, 1, 3, 2, 4)
    spec = spec.reshape(2, scen, A_LEN * sec_local, LANES)
    bands = bands[None, :]
    prob = default_prob[None, :]
    swap = [(n, n ^ 1) for n in range(n_obl)]
    same_core = [[n for n in reversed(range(n_obl)) if n % 2 == c] for c in range(2)]

    next_plane = [(n, n ^ 2) for n in range(n_obl)]
    mine, other = spectral(quantile_index, spec)
    got = lax.ppermute(other, "obl", swap)
    copies = spread(mine, got, tuple(n >> 1 & 1 for n in same_core[0]))
    parts = lax.all_to_all(copies, "obl", 0, 0, axis_index_groups=same_core, tiled=True)
    sums, other_sums = band_weights(live, bands, prob, weights)
    got_sums = lax.ppermute(other_sums, "obl", swap)
    each = (n_sector, sums.shape[0] // n_sector, LANES)
    joined, own = join(parts, sums.reshape(each), got_sums.reshape(each))
    across = lax.ppermute(own, "obl", next_plane)
    near = lax.all_to_all(joined, "sector", 0, 0, tiled=True)
    tables = near[:, : own.shape[0]]
    tables_across = lax.ppermute(tables, "obl", next_plane)
    tables_beside = lax.ppermute(tables, "obl", swap)
    shares = share(own, across, near, n_obl)
    shares = lax.all_to_all(shares, "obl", 0, 0, tiled=True)
    before = lookup(live, tables, tables_beside, bands, prob, weights, None)
    tables_corner = lax.ppermute(tables_across, "obl", swap)
    contrib = lookup(live, tables_across, tables_corner, bands, prob, weights, before)
    total = total_of(shares, sec_local * n_sector / (OBL_DEV * n_sector * n_obl)).T
    return contrib, total


def solution(mesh):
    in_specs = (
        P(None, None, "sector", "obl"),
        P(),
        P(("sector", "obl")),
        P(("sector", "obl")),
        P(None, ("sector", "obl")),
        P("sector", "obl"),
    )
    out_specs = (P(None, ("sector", "obl")), P(None, "sector"))
    return jax.shard_map(
        contributions, mesh=mesh, in_specs=in_specs, out_specs=out_specs, check_vma=False
    )
```

```python
import functools
import math

import jax
import jax.numpy as jnp
from jax import lax
from jax.experimental import pallas as pl
from jax.experimental.pallas import tpu as pltpu
from jax.sharding import PartitionSpec as P


GRID = 65536
BANDS = 1024
OBL_DEV = 1024
LANES = 128
HALF = BANDS // 2
A_LEN = 32
BLOCK = 512
F32 = jnp.float32
BF16 = jnp.bfloat16
I32 = jnp.int32


def iota(shape, dim):
    return lax.broadcasted_iota(I32, shape, dim)


def cos_sin(turns, log_grid):
    quarter_log = log_grid - 2
    quadrant = (turns + (1 << (quarter_log - 1))) >> quarter_log
    rest = turns - (quadrant << quarter_log)
    x = rest.astype(F32) * F32(2.0 * math.pi / (1 << log_grid))
    y = x * x
    sine = x * (1.0 + y * (-1.0 / 6 + y * (1.0 / 120 + y * (-1.0 / 5040 + y * (1.0 / 362880)))))
    cosine = 1.0 + y * (
        -0.5 + y * (1.0 / 24 + y * (-1.0 / 720 + y * (1.0 / 40320 - y * (1.0 / 3628800))))
    )
    odd = (quadrant & 1) == 1
    first = jnp.where(odd, cosine, sine)
    second = jnp.where(odd, sine, cosine)
    return (
        jnp.where(((quadrant + 1) & 2) == 2, -second, second),
        jnp.where((quadrant & 2) == 2, -first, first),
    )


def two_parts(value):
    high = value.astype(BF16).astype(F32)
    return high, value - high


def spectral_kernel(quantile_hbm, spec_hbm, mine, other, quantile, spec, sems, lhs, turn_cos, turn_sin, table, firsts, sums, lines, *grids):
    part = lax.axis_index("obl").astype(I32)
    core = part & 1
    scen = spec.shape[1]
    rows = 2 * scen
    copies = [
        pltpu.make_async_copy(quantile_hbm, quantile, sems.at[0]),
        pltpu.make_async_copy(spec_hbm, spec, sems.at[1]),
    ]
    for copy in copies:
        copy.start()
    shape = (A_LEN, LANES)
    freq = part * (A_LEN * LANES) + iota(shape, 0) * LANES + iota(shape, 1)
    zero = freq == 0
    half_cos, half_sin = cos_sin(freq, 17)
    v_im = jnp.where(zero, 0.0, 0.5 * half_cos / jnp.where(zero, 1.0, half_sin))
    v_re = jnp.where(zero, 0.0, 0.5)
    d_shape = (A_LEN, HALF)
    d_turn = ((part * A_LEN + iota(d_shape, 0)) * iota(d_shape, 1)) & (HALF - 1)
    d_cos, d_sin = cos_sin(d_turn, 9)
    dft = jnp.concatenate(
        [jnp.concatenate([d_cos, -d_sin], 1), jnp.concatenate([d_sin, d_cos], 1)], 0
    )
    d_high, d_low = two_parts(dft)
    d_high = d_high.astype(BF16)
    d_low = d_low.astype(BF16)
    table[...] = jnp.concatenate([d_high, d_high, d_low, d_low], 0)
    t_shape = (LANES, LANES)
    run_cos, run_sin = cos_sin(iota(t_shape, 0) * iota(t_shape, 1), 16)
    step_cos, step_sin = cos_sin(iota(t_shape, 0) * LANES, 16)
    for m in range(8):
        turn_cos[:, m * LANES : (m + 1) * LANES] = run_cos
        turn_sin[:, m * LANES : (m + 1) * LANES] = run_sin
        run_cos, run_sin = (
            run_cos * step_cos - run_sin * step_sin,
            run_sin * step_cos + run_cos * step_sin,
        )
    for copy in copies:
        copy.wait()
    for c in range(scen):
        w_cos, w_sin = cos_sin((freq * (quantile[c] - 1)) & (GRID - 1), 16)
        u_re = v_re * w_cos - v_im * w_sin
        u_im = v_re * w_sin + v_im * w_cos
        for k in range(2):
            x_re = spec[0, c, pl.ds(k, A_LEN, stride=2), :]
            x_im = spec[1, c, pl.ds(k, A_LEN, stride=2), :]
            z_re = x_re * u_re - x_im * u_im
            z_im = x_re * u_im + x_im * u_re
            re_high, re_low = two_parts(z_re)
            im_high, im_low = two_parts(z_im)
            turned = jnp.concatenate([re_high, im_high, re_low, im_low], 0).T.astype(BF16)
            row = k * scen + c
            lhs[row * LANES : (row + 1) * LANES, :LANES] = turned
            lhs[row * LANES : (row + 1) * LANES, LANES:] = turned
            sums[row : row + 1, :] = jnp.sum(x_re * v_re - x_im * v_im, axis=0, keepdims=True)
            firsts[row : row + 1, :] = x_re[0:1, :]
    group = rows // len(grids)
    tiles = HALF // LANES
    for g, grid in enumerate(grids):
        grid[...] = jnp.dot(
            lhs[g * group * LANES : (g + 1) * group * LANES, :],
            table[...],
            preferred_element_type=F32,
        )
        for t in range(tiles):
            lane = t * LANES
            acc = [[None] * group for _ in range(2)]
            for b in range(LANES // 8):
                turn = [
                    (
                        turn_cos[b * 8 : (b + 1) * 8, h * HALF + lane : h * HALF + lane + LANES],
                        turn_sin[b * 8 : (b + 1) * 8, h * HALF + lane : h * HALF + lane + LANES],
                    )
                    for h in range(2)
                ]
                for r in range(group):
                    at = r * LANES + b * 8
                    g_re = grid[at : at + 8, lane : lane + LANES]
                    g_im = grid[at : at + 8, HALF + lane : HALF + lane + LANES]
                    for h in range(2):
                        term = g_re * turn[h][0] + g_im * turn[h][1]
                        acc[h][r] = term if acc[h][r] is None else acc[h][r] + term
            for h in range(2):
                for r in range(group):
                    at = ((h * tiles + t) * rows + g * group + r) * 8
                    lines[at : at + 8, :] = acc[h][r]
    total = jnp.sum(sums[...], axis=1, keepdims=True)
    at_zero = jnp.where(part == 0, firsts[:, 0:1], 0.0)
    lane_at = iota((1, LANES), 1)
    c_of = iota((scen, 1), 0)
    q_less = jnp.zeros((scen, 1), I32)
    for c in range(scen):
        q_less = jnp.where(c_of == c, quantile[c] - 1, q_less)
    for h in range(2):
        for t in range(tiles):
            for k in range(2):
                base = ((h * tiles + t) * rows + k * scen) * 8
                value = lines[pl.ds(base, scen, stride=8), :]
                for s in range(1, 8):
                    value = value + lines[pl.ds(base + s, scen, stride=8), :]
                size = (GRID - q_less + (h * HALF + t * LANES + lane_at)).astype(F32)
                here = slice(k * scen, (k + 1) * scen)
                value = (value + at_zero[here] * size - total[here]) * F32(1.0 / GRID)
                lines[pl.ds(base, scen), :] = value

    def send(h, to):
        for t in range(tiles):
            for k in range(2):
                base = ((h * tiles + t) * rows + k * scen) * 8
                to[t * rows + k * scen : t * rows + (k + 1) * scen, :] = lines[base : base + scen, :]

    @pl.when(core == 0)
    def _():
        send(0, mine)
        send(1, other)

    @pl.when(core == 1)
    def _():
        send(1, mine)
        send(0, other)


def spectral(quantile, spec):
    scen = spec.shape[1]
    rows = 2 * scen
    groups = 4
    hbm = pl.BlockSpec(memory_space=pltpu.HBM)
    vmem = pl.BlockSpec(memory_space=pltpu.VMEM)
    out = jax.ShapeDtypeStruct((HALF // LANES * rows, LANES), F32)
    return pl.pallas_call(
        spectral_kernel,
        out_shape=(out, out),
        in_specs=[hbm, hbm],
        out_specs=(vmem, vmem),
        scratch_shapes=[
            pltpu.SMEM(quantile.shape, I32),
            pltpu.VMEM(spec.shape, F32),
            pltpu.SemaphoreType.DMA((2,)),
            pltpu.VMEM((rows * LANES, 2 * LANES), BF16),
            pltpu.VMEM((LANES, BANDS), F32),
            pltpu.VMEM((LANES, BANDS), F32),
            pltpu.VMEM((2 * LANES, 2 * HALF), BF16),
            pltpu.VMEM((rows, LANES), F32),
            pltpu.VMEM((rows, LANES), F32),
            pltpu.VMEM((BANDS // LANES * rows * 8, LANES), F32),
        ]
        + [pltpu.VMEM((rows // groups * LANES, 2 * HALF), F32)] * groups,
        compiler_params=pltpu.CompilerParams(vmem_limit_bytes=24 << 20),
        cost_estimate=pl.CostEstimate(flops=3_000_000_000, bytes_accessed=600_000, transcendentals=0),
        name="spectral",
    )(
        pltpu.with_memory_space_constraint(quantile, pltpu.HBM),
        pltpu.with_memory_space_constraint(spec, pltpu.HBM),
    )


def slot_factor(bands, prob):
    return prob * bands.astype(F32) / 256.0


def band_weights_kernel(live, bands, prob, weights, mine, other, acc):
    sectors = weights.shape[0]
    width = 2 * BLOCK
    acc[...] = jnp.zeros_like(acc)

    def block(n, _):
        at = pl.multiple_of(n * width, width)
        band = bands[:, pl.ds(at, width)]
        factor = slot_factor(band, prob[:, pl.ds(at, width)])
        alive = at + iota((1, width), 1) < live[0, 0]
        factor = jnp.where(alive, factor, 0.0)
        index = band - 1
        low = index & 255
        high = index >> 8
        value = weights[:, pl.ds(at, width)].astype(F32) * factor
        v_high, v_low = two_parts(value)
        pieces = []
        for h in range(4):
            here = high == h
            pieces.append(jnp.where(here, v_high, 0.0).astype(BF16))
            pieces.append(jnp.where(here, v_low, 0.0).astype(BF16))
        left = jnp.concatenate(pieces, 0)
        hot = (iota((256, width), 0) == low).astype(F32).astype(BF16)
        acc[...] += lax.dot_general(
            left, hot, (((1,), (1,)), ((), ())), preferred_element_type=F32
        )
        return 0

    lax.fori_loop(0, (live[0, 0] + width - 1) // width, block, 0)
    core = lax.axis_index("obl").astype(I32) & 1

    def send(half, to):
        for h in range(2):
            at = (2 * half + h) * 2 * sectors
            both = acc[at : at + sectors, :] + acc[at + sectors : at + 2 * sectors, :]
            for m in range(2):
                chunk = both[:, m * LANES : (m + 1) * LANES]
                to[pl.ds(2 * h + m, sectors, stride=4), :] = chunk

    @pl.when(core == 0)
    def _():
        send(0, mine)
        send(1, other)

    @pl.when(core == 1)
    def _():
        send(1, mine)
        send(0, other)


def band_weights(live, bands, prob, weights):
    sectors = weights.shape[0]
    smem = pl.BlockSpec(memory_space=pltpu.SMEM)
    vmem = pl.BlockSpec(memory_space=pltpu.VMEM)
    out = jax.ShapeDtypeStruct((sectors * HALF // LANES, LANES), F32)
    return pl.pallas_call(
        band_weights_kernel,
        out_shape=(out, out),
        in_specs=[smem, vmem, vmem, vmem],
        out_specs=(vmem, vmem),
        scratch_shapes=[pltpu.VMEM((8 * sectors, 256), F32)],
        compiler_params=pltpu.CompilerParams(vmem_limit_bytes=16 << 20),
        cost_estimate=pl.CostEstimate(flops=600_000_000, bytes_accessed=700_000, transcendentals=0),
        name="band_weights",
    )(live, bands, prob, weights)


def spread_kernel(mine, got, out, *, parities):
    value = mine[...] + got[...]
    rows = out.shape[1]
    for n, parity in enumerate(parities):
        out[n] = value[parity * rows : (parity + 1) * rows]


def spread(mine, got, parities):
    return pl.pallas_call(
        functools.partial(spread_kernel, parities=parities),
        out_shape=jax.ShapeDtypeStruct((len(parities), mine.shape[0] // 2, LANES), F32),
        compiler_params=pltpu.CompilerParams(vmem_limit_bytes=4 << 20),
        name="spread",
    )(mine, got)


def join_kernel(parts, sums, got, out, own, *, order):
    value = parts[0]
    for n in range(1, parts.shape[0]):
        value = value + parts[n]
    rows = value.shape[0]
    own[...] = value
    for n, at in enumerate(order):
        out[n, :rows, :] = value
        out[n, rows:, :] = sums[at] + got[at]


def join(parts, sums, got, order):
    peers, extra, lanes = sums.shape
    rows = parts.shape[1]
    return pl.pallas_call(
        functools.partial(join_kernel, order=order),
        out_shape=(
            jax.ShapeDtypeStruct((peers, rows + extra, lanes), F32),
            jax.ShapeDtypeStruct((rows, lanes), F32),
        ),
        compiler_params=pltpu.CompilerParams(vmem_limit_bytes=4 << 20),
        name="join",
    )(parts, sums, got)


def lookup_kernel(*refs, last, order):
    if last:
        live, same, cross, bands, prob, weights, before, out, lhs = refs
    else:
        live, same, cross, bands, weights, out, lhs = refs
    place = lax.axis_index("obl").astype(I32)
    core = place & 1
    parity = (place >> 1) & 1
    peers = same.shape[0]
    rows = HALF // LANES
    each = 16
    count = peers * each
    sectors = weights.shape[0]
    scen = count // sectors
    for t in range(rows):
        side = same if t < 2 else cross
        at = (t % 2) * each
        value = side[:, at : at + each, :].reshape(count, LANES)
        high, low = two_parts(value)
        lhs[:count, t * LANES : (t + 1) * LANES] = high.astype(BF16)
        lhs[count:, t * LANES : (t + 1) * LANES] = low.astype(BF16)
    want = 1 - parity if last else parity
    step = 4 * BLOCK
    steps = (live[0, 0] + step - 1) // step

    def block(n, _):
        for part in range(4):
            at = pl.multiple_of(n * step + part * BLOCK, BLOCK)
            band = bands[:, pl.ds(at, BLOCK)]
            index = band - 1
            column = (index & 255) + jnp.where((index >> 9) == core, 0, 256)
            column = jnp.where(((index >> 8) & 1) == want, column, -1)
            hot = (iota((HALF, BLOCK), 0) == column).astype(F32).astype(BF16)
            found = jnp.dot(lhs[...], hot, preferred_element_type=F32)
            weight = weights[:, pl.ds(at, BLOCK)].astype(F32)
            acc = jnp.zeros((scen, BLOCK), F32)
            for k in range(sectors):
                entry = found[k * scen : (k + 1) * scen] + found[count + k * scen : count + (k + 1) * scen]
                row = 2 * order[k // 2] + k % 2
                acc = acc + entry * weight[row : row + 1, :]
            if last:
                factor = slot_factor(band, prob[:, pl.ds(at, BLOCK)])
                alive = at + iota((1, BLOCK), 1) < live[0, 0]
                acc = jnp.where(alive, (acc + before[:, pl.ds(at, BLOCK)]) * factor, 0.0)
            out[:, pl.ds(at, BLOCK)] = acc
        return 0

    lax.fori_loop(0, steps, block, 0)
    if last:

        def empty(n, _):
            at = pl.multiple_of(n * step, step)
            out[:, pl.ds(at, step)] = jnp.zeros((out.shape[0], step), F32)
            return 0

        lax.fori_loop(steps, out.shape[1] // step, empty, 0)


def lookup(live, same, cross, bands, prob, weights, before, order):
    last = before is not None
    slots = bands.shape[1]
    sectors = weights.shape[0]
    scen = same.shape[0] * 16 // sectors
    smem = pl.BlockSpec(memory_space=pltpu.SMEM)
    vmem = pl.BlockSpec(memory_space=pltpu.VMEM)
    args = [live, same, cross, bands] + ([prob] if last else []) + [weights] + ([before] if last else [])
    return pl.pallas_call(
        functools.partial(lookup_kernel, last=last, order=order),
        out_shape=jax.ShapeDtypeStruct((scen, slots), F32),
        in_specs=[smem] + [vmem] * (len(args) - 1),
        out_specs=vmem,
        scratch_shapes=[pltpu.VMEM((same.shape[0] * 32, HALF), BF16)],
        compiler_params=pltpu.CompilerParams(vmem_limit_bytes=24 << 20),
        cost_estimate=pl.CostEstimate(flops=4_300_000_000, bytes_accessed=1_000_000, transcendentals=0),
        name="lookup_last" if last else "lookup_first",
    )(*args)


def share_kernel(own, across, near, out):
    parity = (lax.axis_index("obl").astype(I32) >> 1) & 1
    rows = own.shape[0]
    sums = near[0, rows:, :]
    for n in range(1, near.shape[0]):
        sums = sums + near[n, rows:, :]
    acc = [jnp.zeros((8, LANES), F32) for _ in range(2)]
    for t in range(2):
        for k in range(2):
            at = t * 16 + k * 8
            low = sums[k * 4 + t : k * 4 + t + 1, :]
            high = sums[k * 4 + 2 + t : k * 4 + 3 + t, :]
            acc[k] = acc[k] + own[at : at + 8, :] * jnp.where(parity == 0, low, high)
            acc[k] = acc[k] + across[at : at + 8, :] * jnp.where(parity == 0, high, low)
    both = jnp.concatenate(acc + [jnp.zeros((LANES - 16, LANES), F32)], 0).T
    line = jnp.sum(both, axis=0, keepdims=True)
    for n in range(out.shape[0]):
        out[n] = line


def share(own, across, near, copies):
    return pl.pallas_call(
        share_kernel,
        out_shape=jax.ShapeDtypeStruct((copies, 1, LANES), F32),
        compiler_params=pltpu.CompilerParams(vmem_limit_bytes=4 << 20),
        cost_estimate=pl.CostEstimate(flops=1_000_000, bytes_accessed=100_000, transcendentals=0),
        name="share",
    )(own, across, near)


def total_kernel(shares, out, *, scale):
    line = shares[0]
    for n in range(1, shares.shape[0]):
        line = line + shares[n]
    line = line * F32(scale)
    out[0:1, :] = line[:, :8]
    out[1:2, :] = line[:, 8:16]


def total_of(shares, scale):
    return pl.pallas_call(
        functools.partial(total_kernel, scale=scale),
        out_shape=jax.ShapeDtypeStruct((2, 8), F32),
        compiler_params=pltpu.CompilerParams(vmem_limit_bytes=4 << 20),
        name="total",
    )(shares)


def contributions(spectrum, quantile_index, bands, default_prob, weights, live_rows):
    scen, sec_local = spectrum.shape[1], spectrum.shape[2]
    n_obl = lax.axis_size("obl")
    n_sector = lax.axis_size("sector")
    live = live_rows
    spec = spectrum.reshape(2, scen, sec_local, A_LEN, LANES).transpose(0, 1, 3, 2, 4)
    spec = spec.reshape(2, scen, A_LEN * sec_local, LANES)
    bands = bands[None, :]
    prob = default_prob[None, :]
    swap = [(n, n ^ 1) for n in range(n_obl)]
    same_core = [[n for n in reversed(range(n_obl)) if n % 2 == c] for c in range(2)]

    order = tuple(reversed(range(n_sector)))
    next_plane = [(n, n ^ 2) for n in range(n_obl)]
    mine, other = spectral(quantile_index, spec)
    got = lax.ppermute(other, "obl", swap)
    copies = spread(mine, got, tuple(n >> 1 & 1 for n in same_core[0]))
    parts = lax.all_to_all(copies, "obl", 0, 0, axis_index_groups=same_core, tiled=True)
    sums, other_sums = band_weights(live, bands, prob, weights)
    got_sums = lax.ppermute(other_sums, "obl", swap)
    each = (n_sector, sums.shape[0] // n_sector, LANES)
    joined, own = join(parts, sums.reshape(each), got_sums.reshape(each), order)
    across = lax.ppermute(own, "obl", next_plane)
    near = lax.all_to_all(joined, "sector", 0, 0, axis_index_groups=[list(order)], tiled=True)
    tables = near[:, : own.shape[0]]
    tables_across = lax.ppermute(tables, "obl", next_plane)
    tables_beside = lax.ppermute(tables, "obl", swap)
    shares = share(own, across, near, n_obl)
    shares = lax.all_to_all(shares, "obl", 0, 0, axis_index_groups=[[*range(1, n_obl, 2), *range(0, n_obl, 2)]], tiled=True)
    before = lookup(live, tables, tables_beside, bands, prob, weights, None, order)
    tables_corner = lax.ppermute(tables_across, "obl", swap)
    contrib = lookup(live, tables_across, tables_corner, bands, prob, weights, before, order)
    total = total_of(shares, sec_local * n_sector / (OBL_DEV * n_sector * n_obl)).T
    return contrib, total


def solution(mesh):
    in_specs = (
        P(None, None, "sector", "obl"),
        P(),
        P(("sector", "obl")),
        P(("sector", "obl")),
        P(None, ("sector", "obl")),
        P("sector", "obl"),
    )
    out_specs = (P(None, ("sector", "obl")), P(None, "sector"))
    return jax.shard_map(
        contributions, mesh=mesh, in_specs=in_specs, out_specs=out_specs, check_vma=False
    )
```
